128 devices in a mesh: row: 8 (over x, core), col: 16 (over z, y).
Axes of the slice: x: 4, y: 4, z: 4, core: 2. Of those that a mesh axis runs over, the one named last changes fastest.
Arguments:
- voltage: float32 [1024, 4096], P('row', 'col'), may hold values from -6 to 6
- currents: float32 [2, 1024, 4096], P(None, 'row', 'col'), may hold values from -6 to 6
- resistance: float32 [2, 1024, 4096], P(None, 'row', 'col'), may hold values from 0.05 to 0.5
- inverse_cap: float32 [1024, 4096], P('row', 'col'), may hold values from 0.05 to 0.5
- shunt_conductance: float32 [1024, 4096], P('row', 'col'), may hold values from 0.1 to 1
- tap_index: int32 [1024, 4096], P('row', 'col'), may hold values from 0 to 8
- pad_mask: int32 [1024, 4096], P('row', 'col'), may hold values 0 or 1
- waveforms: float32 [2, 8], replicated, may hold values from -8 to 8
- k_window: bfloat16 [2, 33, 33], replicated, may hold values from -0.1 to 0.4
Outputs:
- voltage_out: float32 [1024, 4096], P('row', 'col')
- current_out: float32 [2, 1024, 4096], P(None, 'row', 'col')
The draws below stay inside these ranges and needn't reach their ends.
All inputs are finite; a program needn't handle non-finite values. No bound on the sum of `pad_mask` on one device may be relied on, other than what follows from the above.
Results may differ from the reference program's by a relative error of at most 0.0023.
Values may be sent and summed in bfloat16 or wider, within the bound.
A program may use at most 64 MiB of HBM per device.

```python
import math
import jax
import jax.numpy as jnp
from jax import lax

CY = 256
HALF = 16
STEPS = 2
NW = 8
NX = 1024
NY = 4096


def draw_k_window(key, part):
    window_span = 2 * HALF + 1
    noise = jax.random.normal(key, (2, window_span, window_span), jnp.float32) * 0.012
    noise = jnp.clip(noise, -0.09, 0.09)
    center = jnp.zeros((2, window_span, window_span), jnp.float32).at[:, HALF, HALF].set(0.3)
    return (noise + center).astype(jnp.bfloat16)


def with_ends(values, key, least, top_value):
    spot = [jax.random.randint(jax.random.fold_in(key, axis), (), 0, length) for axis, length in enumerate(values.shape)]
    main_axis = values.shape.index(max(values.shape))
    neighbour = spot[:main_axis] + [(spot[main_axis] + 1) % values.shape[main_axis]] + spot[main_axis + 1:]
    return values.at[tuple(spot)].set(least).at[tuple(neighbour)].set(top_value)


def block_scale(own_key, shape, cuts, low, high):
    loudness, own = 1.0, jax.random.fold_in(own_key, 6)
    for position, parts in cuts:
        draws = jnp.exp(jax.random.uniform(jax.random.fold_in(own, position), (parts,), jnp.float32, low / len(cuts), high / len(cuts)))
        loudness = loudness * jnp.repeat(draws, shape[position] // parts).reshape([-1 if axis == position else 1 for axis in range(len(shape))])
    return loudness


def bell_draw(rng, shape, scale, reach, split=(), held_as=jnp.bfloat16):
    drawn = scale * jax.random.normal(rng, shape, jnp.float32)
    if split:
        drawn = drawn * block_scale(rng, shape, split, -0.22, 0.18)
    return jnp.clip(drawn, -reach, reach).astype(held_as)


def setup_inputs(seed: int = 0) -> dict:
    arg_keys = jax.random.split(jax.random.key(seed), 10)
    return {
        "voltage": bell_draw(arg_keys[0], (NX, NY), 1.0, 6.0, ((0, 8), (1, 16)), jnp.float32),
        "currents": bell_draw(arg_keys[1], (2, NX, NY), 1.0, 6.0, ((1, 8), (2, 16)), jnp.float32),
        "resistance": jnp.clip(jnp.exp(math.log(0.5) - 2.3025851 * jax.random.uniform(arg_keys[2], (2, NX, NY), jnp.float32) ** block_scale(arg_keys[2], (2, NX, NY), ((1, 8), (2, 16)), -0.2, 0.2)), 0.05, 0.5),
        "inverse_cap": jnp.clip(jnp.exp(math.log(0.5) - 2.3025851 * jax.random.uniform(arg_keys[3], (NX, NY), jnp.float32) ** block_scale(arg_keys[3], (NX, NY), ((0, 8), (1, 16)), -0.2, 0.2)), 0.05, 0.5),
        "shunt_conductance": jnp.clip(jnp.exp(math.log(1.0) - 2.3025851 * jax.random.uniform(arg_keys[4], (NX, NY), jnp.float32) ** block_scale(arg_keys[4], (NX, NY), ((0, 8), (1, 16)), -0.2, 0.2)), 0.1, 1.0),
        "tap_index": with_ends(jax.random.randint(arg_keys[5], (NX, NY), 0, NW + 1), jax.random.fold_in(arg_keys[5], 1), 0, NW).astype(jnp.int32),
        "pad_mask": with_ends((jax.random.randint(arg_keys[6], (NX, NY), 0, 16) < 1).astype(jnp.int32), jax.random.fold_in(arg_keys[6], 1), 0, 1),
        "waveforms": bell_draw(arg_keys[7], (STEPS, NW), 2.0, 8.0, (), jnp.float32),
        "k_window": draw_k_window(jax.random.fold_in(arg_keys[9], 71), 0),
    }


def toeplitz_rows(kernel_row, width_in, width_out):
    window_span = kernel_row.shape[1]
    in_index = jnp.arange(width_in, dtype=jnp.int32)[:, None]
    out_index = jnp.arange(width_out, dtype=jnp.int32)[None, :]
    offsets_col = in_index - out_index
    inside = (offsets_col >= 0) & (offsets_col < window_span)
    entries = jnp.take(kernel_row, jnp.clip(offsets_col, 0, window_span - 1), axis=1)
    return jnp.where(inside[None], entries, jnp.zeros_like(entries))


def window_apply(padded, kernel, row_count, col_count):
    window_span = kernel.shape[1]

    def accumulate(offset, running):
        row_slab = lax.dynamic_slice_in_dim(padded, offset, row_count, 1)
        kernel_row = lax.dynamic_index_in_dim(kernel, offset, 1, keepdims=False)
        matrix = toeplitz_rows(kernel_row, col_count + window_span - 1, col_count)
        return running + jnp.einsum("crj,cjk->crk", row_slab, matrix, preferred_element_type=jnp.float32)

    start = jnp.zeros((2, row_count, col_count), jnp.float32)
    return lax.fori_loop(0, window_span, accumulate, start)


def loads_of(tap_index, wave_row):
    running = jnp.zeros(tap_index.shape, jnp.float32)
    for which in range(NW):
        running = running + jnp.where(tap_index == which, wave_row[which], jnp.float32(0.0))
    return running


def reference(voltage, currents, resistance, inverse_cap, shunt_conductance, tap_index, pad_mask, waveforms, k_window):
    blocks = NY // CY
    for step_index in range(STEPS):
        shifted = jnp.pad(voltage, ((0, 1), (0, 1)))
        drop_pair = jnp.stack([voltage - shifted[1:, :-1], voltage - shifted[:-1, 1:]])
        driving = (drop_pair - resistance * currents).astype(jnp.bfloat16)
        padded = jnp.pad(driving, ((0, 0), (HALF, HALF), (HALF, HALF)))

        def one_block(block):
            col_slab = lax.dynamic_slice(padded, (jnp.int32(0), jnp.int32(0), block * CY), (2, NX + 2 * HALF, CY + 2 * HALF))
            return window_apply(col_slab, k_window, NX, CY)

        pieces = lax.map(one_block, jnp.arange(blocks, dtype=jnp.int32))
        update = jnp.transpose(pieces, (1, 2, 0, 3)).reshape(2, NX, NY)
        currents = currents + update
        before_x = jnp.pad(currents[0], ((1, 0), (0, 0)))[:-1]
        before_y = jnp.pad(currents[1], ((0, 0), (1, 0)))[:, :-1]
        divergence = currents[0] - before_x + currents[1] - before_y
        load = loads_of(tap_index, waveforms[step_index])
        voltage = voltage + inverse_cap * (load - divergence - shunt_conductance * voltage)
        voltage = jnp.where(pad_mask == 1, jnp.float32(0.0), voltage)
    return voltage, currents
```

```python
import functools

import jax
import jax.numpy as jnp
from jax import lax
from jax.experimental import pallas as pl
from jax.experimental.pallas import tpu as pltpu
from jax.sharding import PartitionSpec as P

HALF = 16
SPAN = 2 * HALF + 1
STEPS = 2
NW = 8
ROWS = 128
COLS = 256
LANES = 128
TOP = 24
EXT = ROWS + 2 * TOP
DEEP = EXT + 24
GROUP = 4
TAPS = SPAN + GROUP - 1
DEPTH = TAPS * LANES
MESH = pl.DeviceIdType.MESH
F32 = jnp.float32
BF16 = jnp.bfloat16
DIRECTIONS = ((-1, 0), (1, 0), (0, -1), (0, 1), (-1, -1), (-1, 1), (1, -1), (1, 1))


def lane_of(shape):
    return lax.broadcasted_iota(jnp.int32, shape, len(shape) - 1)


def roll(value, amount):
    return pltpu.roll(value, amount % LANES, 1)


def packed(first, second, third, fourth):
    lane = lane_of(first.shape)
    return jnp.where(lane < 32, first, jnp.where(lane < 64, second, jnp.where(lane < 96, third, fourth)))


def one_if(flag):
    return jnp.where(flag, 1, 0)


def build_table(k_ref, comp, pad_ref, base_ref, table_ref):
    pad_ref[...] = jnp.zeros_like(pad_ref)
    pad_ref[8 : 8 + SPAN, 0:SPAN] = k_ref[:, comp, :].astype(F32)
    tap = lax.broadcasted_iota(jnp.int32, (LANES, LANES), 0)
    lane = lax.broadcasted_iota(jnp.int32, (LANES, LANES), 1)
    near = jnp.where(((HALF - tap) & 127) == lane, 1.0, 0.0).astype(BF16)
    far = jnp.where(((HALF + 64 - tap) & 127) == lane, 1.0, 0.0).astype(BF16)
    near = jnp.where(tap < SPAN, near, jnp.zeros_like(near))
    far = jnp.where(tap < SPAN, far, jnp.zeros_like(far))
    here = pad_ref[8:48, :].astype(BF16)
    above = pad_ref[7:47, :].astype(BF16)
    base_ref[...] = jnp.dot(here, near, preferred_element_type=F32) + jnp.dot(above, far, preferred_element_type=F32)
    inside = ((tap - (lane & 63) + HALF) & 127) < SPAN

    def one(index, carry):
        row = jnp.broadcast_to(base_ref[pl.ds(index, 1), :], (LANES, LANES))
        turned = pltpu.roll(row, 0, 1, stride=1, stride_axis=0)
        block = jnp.where(inside, turned, 0.0).astype(BF16)
        table_ref[comp, pl.ds(pl.multiple_of(index * LANES, LANES), LANES), 0:LANES] = block
        table_ref[comp, pl.ds(pl.multiple_of((index + 2) * LANES, LANES), LANES), LANES:] = block
        return carry

    lax.fori_loop(0, SPAN + 1, one, 0)
    blank = jnp.zeros((2 * LANES, LANES), BF16)
    table_ref[comp, (SPAN + 1) * LANES :, 0:LANES] = blank
    table_ref[comp, 0 : 2 * LANES, LANES:] = blank


def kernel(
    wave_hbm, k_hbm, v_hbm, c_hbm, r_hbm, cap_hbm, shunt_hbm, tap_hbm, mask_hbm,
    vout_ref, cout_ref,
    r_ref, cap_ref, shunt_ref, tap_ref, mask_ref,
    frame_ref, cur0_ref, cur1_ref, curl_ref,
    sendl_ref, sendr_ref, fromr_ref, froml_ref,
    drive_ref, lhs_ref, table_ref, pad_ref, base_ref, load_ref,
    flow0_ref, flow1_ref, flowl_ref,
    wave_ref, k_ref, load_sem, send_sem, recv_sem, cur_sem,
):
    my_row, my_col = lax.axis_index("row"), lax.axis_index("col")
    n_row, n_col = lax.axis_size("row"), lax.axis_size("col")

    def exists(dr, dc):
        row, col = my_row + dr, my_col + dc
        ok = None
        for spot, count, delta in ((row, n_row, dr), (col, n_col, dc)):
            if delta:
                here = (spot >= 0) & (spot < count)
                ok = here if ok is None else ok & here
        return ok

    loads = [
        pltpu.make_async_copy(v_hbm, frame_ref.at[0, 0, pl.ds(TOP, ROWS), :], load_sem.at[0]),
        pltpu.make_async_copy(c_hbm.at[0], cur0_ref.at[pl.ds(8, ROWS), :], load_sem.at[1]),
        pltpu.make_async_copy(c_hbm.at[1], cur1_ref, load_sem.at[2]),
        pltpu.make_async_copy(r_hbm, r_ref, load_sem.at[3]),
        pltpu.make_async_copy(cap_hbm, cap_ref, load_sem.at[4]),
        pltpu.make_async_copy(shunt_hbm, shunt_ref, load_sem.at[5]),
        pltpu.make_async_copy(tap_hbm, tap_ref, load_sem.at[6]),
        pltpu.make_async_copy(mask_hbm, mask_ref, load_sem.at[7]),
        pltpu.make_async_copy(k_hbm, k_ref, load_sem.at[8]),
        pltpu.make_async_copy(wave_hbm, wave_ref, load_sem.at[9]),
    ]
    for one in loads:
        one.start()
    barrier = pltpu.get_barrier_semaphore()
    for dr, dc in DIRECTIONS:
        @pl.when(exists(dr, dc))
        def _(dr=dr, dc=dc):
            pl.semaphore_signal(barrier, inc=1, device_id=(my_row + dr, my_col + dc), device_id_type=MESH)

    has_up, has_down, has_left, has_right = (exists(*d) for d in DIRECTIONS[:4])

    for step in range(STEPS):
        @pl.when(jnp.logical_not(has_up))
        def _(step=step):
            frame_ref[step, :, 0:TOP, :] = jnp.zeros((3, TOP, COLS), F32)
            froml_ref[step, 0:TOP, :] = jnp.zeros((TOP, LANES), F32)
            fromr_ref[step, 0:TOP, :] = jnp.zeros((TOP, LANES), F32)

        @pl.when(jnp.logical_not(has_down))
        def _(step=step):
            frame_ref[step, :, TOP + ROWS :, :] = jnp.zeros((3, TOP, COLS), F32)
            froml_ref[step, TOP + ROWS :, :] = jnp.zeros((TOP, LANES), F32)
            fromr_ref[step, TOP + ROWS :, :] = jnp.zeros((TOP, LANES), F32)

        @pl.when(jnp.logical_not(has_left))
        def _(step=step):
            froml_ref[step] = jnp.zeros((EXT, LANES), F32)

        @pl.when(jnp.logical_not(has_right))
        def _(step=step):
            fromr_ref[step] = jnp.zeros((EXT, LANES), F32)

    @pl.when(jnp.logical_not(has_up))
    def _():
        cur0_ref[0:8, :] = jnp.zeros((8, COLS), F32)

    def message(step, which):
        frame, left, right = frame_ref.at[step], sendl_ref.at[step], sendr_ref.at[step]
        to_right, to_left = froml_ref.at[step], fromr_ref.at[step]
        low, mid, high = pl.ds(0, TOP), pl.ds(TOP, ROWS), pl.ds(TOP + ROWS, TOP)
        first, last = pl.ds(0, TOP), pl.ds(ROWS - TOP, TOP)
        source, target = (
            (frame.at[:, pl.ds(TOP, TOP), :], frame.at[:, high, :]),
            (frame.at[:, pl.ds(ROWS, TOP), :], frame.at[:, low, :]),
            (left, to_left.at[mid, :]),
            (right, to_right.at[mid, :]),
            (left.at[first, :], to_left.at[high, :]),
            (right.at[first, :], to_right.at[high, :]),
            (left.at[last, :], to_left.at[low, :]),
            (right.at[last, :], to_right.at[low, :]),
        )[which]
        dr, dc = DIRECTIONS[which]
        return pltpu.make_async_remote_copy(
            src_ref=source,
            dst_ref=target,
            send_sem=send_sem.at[step, which],
            recv_sem=recv_sem.at[step, which],
            device_id=(my_row + dr, my_col + dc),
            device_id_type=MESH,
        )

    edge = pltpu.make_async_remote_copy(
        src_ref=cur0_ref.at[pl.ds(ROWS, 8), :],
        dst_ref=cur0_ref.at[pl.ds(0, 8), :],
        send_sem=cur_sem.at[0],
        recv_sem=cur_sem.at[1],
        device_id=(my_row + 1, my_col),
        device_id_type=MESH,
    )

    def fill_products(step, lo, n):
        rows = pl.ds(TOP + lo, n)
        v = frame_ref[step, 0, rows, :]
        c1 = cur1_ref[pl.ds(lo, n), :]
        w0 = r_ref[0, pl.ds(lo, n), :] * cur0_ref[pl.ds(8 + lo, n), :]
        w1 = r_ref[1, pl.ds(lo, n), :] * c1
        frame_ref[step, 1, rows, :] = w0
        frame_ref[step, 2, rows, :] = w1
        a, b = slice(0, LANES), slice(LANES, COLS)
        sendl_ref[step, pl.ds(lo, n), :] = packed(v[:, a], roll(w0[:, a], 32), roll(w1[:, a], 64), w1[:, a])
        sendr_ref[step, pl.ds(lo, n), :] = packed(roll(v[:, b], 32), roll(w0[:, b], 64), roll(w1[:, b], 96), c1[:, b])

    def send(step):
        for which, (dr, dc) in enumerate(DIRECTIONS):
            @pl.when(exists(dr, dc))
            def _(which=which):
                message(step, which).start()

    def receive(step):
        for which, (dr, dc) in enumerate(DIRECTIONS):
            @pl.when(exists(-dr, -dc))
            def _(which=which):
                message(step, which).wait_recv()

    def drain(step):
        for which, (dr, dc) in enumerate(DIRECTIONS):
            @pl.when(exists(dr, dc))
            def _(which=which):
                message(step, which).wait_send()

    def drive(step):
        lo = jnp.where(has_up, 0, TOP)
        hi = jnp.where(has_down, EXT, TOP + ROWS)
        n = 56
        for base in range(0, EXT - 8, n):
            at, nxt = pl.ds(base, n), pl.ds(base + 1, n)
            row = lax.broadcasted_iota(jnp.int32, (n, LANES), 0) + base
            lane = lane_of((n, LANES))
            inside = (row >= lo) & (row < hi)
            left, left_next = froml_ref[step, at, :], froml_ref[step, nxt, :]
            right, right_next = fromr_ref[step, at, :], fromr_ref[step, nxt, :]
            tiles = [slice(0, LANES), slice(LANES, COLS)]
            v = [roll(left, 96)] + [frame_ref[step, 0, at, t] for t in tiles] + [right]
            below = [roll(left_next, 96)] + [frame_ref[step, 0, nxt, t] for t in tiles] + [right_next]
            w0 = [roll(left, 64)] + [frame_ref[step, 1, at, t] for t in tiles] + [roll(right, 96)]
            w1 = [roll(left, 32)] + [frame_ref[step, 2, at, t] for t in tiles] + [roll(right, 64)]
            held = [inside & has_left, inside, inside, inside & has_right]
            for comp in range(2):
                out = []
                for k in range(4):
                    if comp == 0:
                        value = v[k] - below[k] - w0[k]
                    else:
                        follow = v[min(k + 1, 3)]
                        beside = roll(jnp.where(lane == 0, follow, v[k]), 127)
                        value = v[k] - beside - w1[k]
                    out.append(jnp.where(held[k], value, 0.0))
                tl, ta, tb, tr = out
                slot = 4 * comp
                drive_ref[slot, at, :] = jnp.where(lane < 96, ta, tl)
                drive_ref[slot + 1, at, :] = roll(jnp.where(lane < 32, tb, ta), 64)
                drive_ref[slot + 2, at, :] = jnp.where(lane < 96, tb, ta)
                drive_ref[slot + 3, at, :] = roll(jnp.where(lane < 32, tr, tb), 64)
                if comp == 1:
                    drive_ref[8, at, :] = roll(jnp.where(lane < 64, ta, tl), 64)

    def convolve(comp):
        slots, start, n = ((0, 1, 2, 3), 4, 40) if comp == 0 else ((4, 5, 6, 7, 8), 8, 32)
        for tap in range(TAPS):
            pieces = [drive_ref[slot, pl.ds(start + tap, n, stride=GROUP), :] for slot in slots]
            lhs_ref[:, tap * LANES : (tap + 1) * LANES] = jnp.concatenate(pieces, axis=0).astype(BF16)
        product = jnp.dot(lhs_ref[...], table_ref[comp], preferred_element_type=F32)
        low = lane_of((n, LANES)) < 64
        for t in range(GROUP):
            half = product[:, (t // 2) * LANES : (t // 2 + 1) * LANES]
            part = [half[i * n : (i + 1) * n] for i in range(len(slots))]
            for p in range(2):
                even, odd = part[2 * p], part[2 * p + 1]
                if t % 2 == 0:
                    tile = jnp.where(low, even, roll(odd, 64))
                else:
                    tile = jnp.where(low, roll(even, 64), odd)
                cols = slice(p * LANES, (p + 1) * LANES)
                if comp == 0:
                    flow0_ref[p, pl.ds(4 + t, n, stride=GROUP), :] = tile
                else:
                    flow1_ref[p, pl.ds(t, n, stride=GROUP), :] = tile
            if comp == 1:
                flowl_ref[pl.ds(t, n, stride=GROUP), :] = roll(part[4], 64) if t % 2 == 0 else part[4]

    def advance(step):
        for p in range(2):
            cols = slice(p * LANES, (p + 1) * LANES)
            head = cur0_ref[0:8, cols] + flow0_ref[p, 0:8, :]
            cur0_ref[0:8, cols] = jnp.where(has_up, head, 0.0)
        n = 32
        for lo in range(0, ROWS, n):
            rows = pl.ds(lo, n)
            for p in range(2):
                cols = slice(p * LANES, (p + 1) * LANES)
                cur0_ref[pl.ds(8 + lo, n), cols] = cur0_ref[pl.ds(8 + lo, n), cols] + flow0_ref[p, pl.ds(8 + lo, n), :]
                cur1_ref[rows, cols] = cur1_ref[rows, cols] + flow1_ref[p, rows, :]
            curl_ref[rows, :] = jnp.where(has_left, curl_ref[rows, :] + flowl_ref[rows, :], 0.0)

    def update(step, target):
        n = 32
        for lo in range(0, ROWS, n):
            rows = pl.ds(lo, n)
            lane = lane_of((n, LANES))
            c1 = [curl_ref[rows, :], cur1_ref[rows, 0:LANES], cur1_ref[rows, LANES:]]
            for p in range(2):
                cols = slice(p * LANES, (p + 1) * LANES)
                c0 = cur0_ref[pl.ds(8 + lo, n), cols]
                before_x = cur0_ref[pl.ds(7 + lo, n), cols]
                before_y = roll(jnp.where(lane == LANES - 1, c1[p], c1[p + 1]), 1)
                divergence = c0 - before_x + c1[p + 1] - before_y
                v = frame_ref[step, 0, pl.ds(TOP + lo, n), cols]
                new = v + cap_ref[rows, cols] * (load_ref[step, rows, cols] - divergence - shunt_ref[rows, cols] * v)
                target(lo, n, cols, jnp.where(mask_ref[rows, cols] == 1, 0.0, new))

    def fill_loads():
        n = 32
        for lo in range(0, ROWS, n):
            rows = pl.ds(lo, n)
            tap = tap_ref[rows, :]
            for step in range(STEPS):
                value = jnp.zeros(tap.shape, F32)
                for which in range(NW):
                    value = jnp.where(tap == which, wave_ref[step, which], value)
                load_ref[step, rows, :] = value

    for one in loads[:4]:
        one.wait()
    for lo in range(0, ROWS, 32):
        fill_products(0, lo, 32)
    pl.semaphore_wait(barrier, (1 + one_if(has_up) + one_if(has_down)) * (1 + one_if(has_left) + one_if(has_right)) - 1)
    send(0)

    @pl.when(has_down)
    def _():
        edge.start()

    for one in loads[4:]:
        one.wait()
    build_table(k_ref, 0, pad_ref, base_ref, table_ref)
    build_table(k_ref, 1, pad_ref, base_ref, table_ref)
    fill_loads()

    @pl.when(has_down)
    def _():
        edge.wait_send()

    @pl.when(has_up)
    def _():
        edge.wait_recv()

    for step in range(STEPS):
        receive(step)
        if step == 0:
            curl_ref[...] = froml_ref[0, TOP : TOP + ROWS, :]
        drive(step)
        convolve(0)
        convolve(1)
        advance(step)
        if step + 1 < STEPS:
            def keep(lo, n, cols, value, step=step):
                frame_ref[step + 1, 0, pl.ds(TOP + lo, n), cols] = value

            update(step, keep)
            for lo in range(0, ROWS, 32):
                fill_products(step + 1, lo, 32)
            send(step + 1)
        else:
            def keep_last(lo, n, cols, value):
                vout_ref[pl.ds(lo, n), cols] = value

            cout_ref[0] = cur0_ref[8 : 8 + ROWS, :]
            cout_ref[1] = cur1_ref[...]
            update(step, keep_last)
    for step in range(STEPS):
        drain(step)


def local(voltage, currents, resistance, inverse_cap, shunt_conductance, tap_index, pad_mask, waveforms, k_window):
    anywhere = pl.BlockSpec(memory_space=pltpu.HBM)
    vmem = pl.BlockSpec(memory_space=pltpu.VMEM)
    block = (ROWS, COLS)
    scratch = [
        pltpu.VMEM((2, *block), F32),
        pltpu.VMEM(block, F32),
        pltpu.VMEM(block, F32),
        pltpu.VMEM(block, jnp.int32),
        pltpu.VMEM(block, jnp.int32),
        pltpu.VMEM((STEPS, 3, EXT, COLS), F32),
        pltpu.VMEM((ROWS + 8, COLS), F32),
        pltpu.VMEM(block, F32),
        pltpu.VMEM((ROWS, LANES), F32),
        pltpu.VMEM((STEPS, ROWS, LANES), F32),
        pltpu.VMEM((STEPS, ROWS, LANES), F32),
        pltpu.VMEM((STEPS, EXT, LANES), F32),
        pltpu.VMEM((STEPS, EXT, LANES), F32),
        pltpu.VMEM((9, DEEP, LANES), F32),
        pltpu.VMEM((160, DEPTH), BF16),
        pltpu.VMEM((2, DEPTH, 2 * LANES), BF16),
        pltpu.VMEM((48, LANES), F32),
        pltpu.VMEM((40, LANES), F32),
        pltpu.VMEM((STEPS, *block), F32),
        pltpu.VMEM((2, ROWS + 40, LANES), F32),
        pltpu.VMEM((2, ROWS, LANES), F32),
        pltpu.VMEM((ROWS, LANES), F32),
        pltpu.SMEM((STEPS, NW), F32),
        pltpu.VMEM((SPAN, 2, SPAN), BF16),
        pltpu.SemaphoreType.DMA((10,)),
        pltpu.SemaphoreType.DMA((STEPS, 8)),
        pltpu.SemaphoreType.DMA((STEPS, 8)),
        pltpu.SemaphoreType.DMA((2,)),
    ]
    call = pl.pallas_call(
        kernel,
        out_shape=(jax.ShapeDtypeStruct(block, F32), jax.ShapeDtypeStruct((2, *block), F32)),
        in_specs=[anywhere] * 9,
        out_specs=(vmem, vmem),
        scratch_shapes=scratch,
        compiler_params=pltpu.CompilerParams(
            collective_id=0, has_side_effects=True, vmem_limit_bytes=40 * 1024 * 1024
        ),
    )
    held = [waveforms, jnp.transpose(k_window, (1, 0, 2)), voltage, currents, resistance, inverse_cap]
    held += [shunt_conductance, tap_index, pad_mask]
    held = [pltpu.with_memory_space_constraint(one, pltpu.HBM) for one in held]
    return call(*held)


def solution(mesh):
    placed = (
        P("row", "col"),
        P(None, "row", "col"),
        P(None, "row", "col"),
        P("row", "col"),
        P("row", "col"),
        P("row", "col"),
        P("row", "col"),
        P(),
        P(),
    )
    return jax.shard_map(
        local,
        mesh=mesh,
        in_specs=placed,
        out_specs=(P("row", "col"), P(None, "row", "col")),
        check_vma=False,
    )
```

```python
import functools

import jax
import jax.numpy as jnp
from jax import lax
from jax.experimental import pallas as pl
from jax.experimental.pallas import tpu as pltpu
from jax.sharding import PartitionSpec as P

HALF = 16
SPAN = 2 * HALF + 1
STEPS = 2
NW = 8
ROWS = 128
COLS = 256
LANES = 128
TOP = 48
EXT = ROWS + 2 * TOP
SKIP = 8
DEEP = 232
WIDE = 34
NEAR = 18
FLOW = 200
FROM = 24
GROUP = 4
TAPS = SPAN + GROUP - 1
DEPTH = TAPS * LANES
MESH = pl.DeviceIdType.MESH
F32 = jnp.float32
BF16 = jnp.bfloat16
DIRECTIONS = ((-1, 0), (1, 0), (0, -1), (0, 1), (-1, -1), (-1, 1), (1, -1), (1, 1))


def lane_of(shape):
    return lax.broadcasted_iota(jnp.int32, shape, len(shape) - 1)


def roll(value, amount):
    return pltpu.roll(value, amount % LANES, 1)


def one_if(flag):
    return jnp.where(flag, 1, 0)


def build_table(k_ref, comp, pad_ref, base_ref, table_ref):
    pad_ref[...] = jnp.zeros_like(pad_ref)
    pad_ref[8 : 8 + SPAN, 0:SPAN] = k_ref[:, comp, :].astype(F32)
    tap = lax.broadcasted_iota(jnp.int32, (LANES, LANES), 0)
    lane = lax.broadcasted_iota(jnp.int32, (LANES, LANES), 1)
    near = jnp.where(((HALF - tap) & 127) == lane, 1.0, 0.0).astype(BF16)
    far = jnp.where(((HALF + 64 - tap) & 127) == lane, 1.0, 0.0).astype(BF16)
    near = jnp.where(tap < SPAN, near, jnp.zeros_like(near))
    far = jnp.where(tap < SPAN, far, jnp.zeros_like(far))
    here = pad_ref[8:48, :].astype(BF16)
    above = pad_ref[7:47, :].astype(BF16)
    base_ref[...] = jnp.dot(here, near, preferred_element_type=F32) + jnp.dot(above, far, preferred_element_type=F32)
    inside = ((tap - (lane & 63) + HALF) & 127) < SPAN

    def one(index, carry):
        row = jnp.broadcast_to(base_ref[pl.ds(index, 1), :], (LANES, LANES))
        turned = pltpu.roll(row, 0, 1, stride=1, stride_axis=0)
        block = jnp.where(inside, turned, 0.0).astype(BF16)
        table_ref[comp, pl.ds(pl.multiple_of(index * LANES, LANES), LANES), 0:LANES] = block
        table_ref[comp, pl.ds(pl.multiple_of((index + 2) * LANES, LANES), LANES), LANES:] = block
        return carry

    lax.fori_loop(0, SPAN + 1, one, 0)
    blank = jnp.zeros((2 * LANES, LANES), BF16)
    table_ref[comp, (SPAN + 1) * LANES :, 0:LANES] = blank
    table_ref[comp, 0 : 2 * LANES, LANES:] = blank


SLOTS = (("vh", WIDE), ("vl", WIDE), ("w0", WIDE), ("w1", WIDE), ("c0", NEAR), ("c1", NEAR), ("r0", NEAR), ("r1", NEAR), ("b", NEAR), ("q", NEAR))
ROW_BASE = {name: sum(width for _, width in SLOTS[:i]) for i, (name, _) in enumerate(SLOTS)}
WIDTH = dict(SLOTS)
LANE_TILES = (("vh", "vl", "w0", "q"), ("w1", "c0", "c1", "r0", "r1", "b"))


def lane_slots(names):
    base = 0
    for name in names:
        yield name, base
        base += WIDTH[name]


def kernel(
    wave_hbm, k_hbm, v_hbm, c_hbm, r_hbm, cap_hbm, shunt_hbm, tap_hbm, mask_hbm,
    vout_ref, cout_ref,
    cap_ref, shunt_ref, tap_ref, mask_ref,
    v_ref, w_ref, c_ref, r_ref, b_ref, q_ref,
    stage_ref, sendv_ref, sends_ref, fromv_ref, froms_ref,
    drive_ref, lhs_ref, table_ref, pad_ref, base_ref, load_ref, flow_ref,
    wave_ref, k_ref, load_sem, send_sem, recv_sem,
):
    my_row, my_col = lax.axis_index("row"), lax.axis_index("col")
    n_row, n_col = lax.axis_size("row"), lax.axis_size("col")

    def exists(dr, dc):
        row, col = my_row + dr, my_col + dc
        ok = None
        for spot, count, delta in ((row, n_row, dr), (col, n_col, dc)):
            if delta:
                here = (spot >= 0) & (spot < count)
                ok = here if ok is None else ok & here
        return ok

    own = pl.ds(TOP, ROWS)
    pairs = [(k_hbm, k_ref), (wave_hbm, wave_ref)]
    pairs += [(cap_hbm, cap_ref), (shunt_hbm, shunt_ref), (tap_hbm, tap_ref), (mask_hbm, mask_ref)]
    for p in range(2):
        cols = pl.ds(p * LANES, LANES)
        pairs.append((v_hbm.at[:, cols], v_ref.at[p + 1, own, :]))
        for comp in range(2):
            pairs.append((c_hbm.at[comp, :, cols], c_ref.at[comp, p + 1, own, :]))
            pairs.append((r_hbm.at[comp, :, cols], r_ref.at[comp, p + 1, own, :]))
    loads = [pltpu.make_async_copy(src, dst, load_sem.at[i]) for i, (src, dst) in enumerate(pairs)]
    for one in loads:
        one.start()
    barrier = pltpu.get_barrier_semaphore()
    for dr, dc in DIRECTIONS:
        @pl.when(exists(dr, dc))
        def _(dr=dr, dc=dc):
            pl.semaphore_signal(barrier, inc=1, device_id=(my_row + dr, my_col + dc), device_id_type=MESH)

    has_up, has_down, has_left, has_right = (exists(*d) for d in DIRECTIONS[:4])

    for side, missing in enumerate((has_up, has_down)):
        @pl.when(jnp.logical_not(missing))
        def _(side=side):
            fromv_ref[side] = jnp.zeros(fromv_ref.shape[1:], BF16)
            rows = pl.ds(0, TOP) if side == 0 else pl.ds(TOP + ROWS, TOP)
            for other in range(2):
                froms_ref[other, rows, :] = jnp.zeros((TOP, COLS), BF16)

    for side, missing in enumerate((has_left, has_right)):
        @pl.when(jnp.logical_not(missing))
        def _(side=side):
            froms_ref[side] = jnp.zeros(froms_ref.shape[1:], BF16)

    def message(which):
        dr, dc = DIRECTIONS[which]
        low, mid, high = pl.ds(0, TOP), pl.ds(TOP, ROWS), pl.ds(TOP + ROWS, TOP)
        first, last = pl.ds(0, TOP), pl.ds(ROWS - TOP, TOP)
        if dc == 0:
            side = 0 if dr > 0 else 1
            source, target = sendv_ref.at[1 - side], fromv_ref.at[side]
        else:
            side = 0 if dc > 0 else 1
            out, land = sends_ref.at[1 - side], froms_ref.at[side]
            source = out if dr == 0 else out.at[first if dr < 0 else last, :]
            target = land.at[mid if dr == 0 else (high if dr < 0 else low), :]
        return pltpu.make_async_remote_copy(
            src_ref=source,
            dst_ref=target,
            send_sem=send_sem.at[which],
            recv_sem=recv_sem.at[which],
            device_id=(my_row + dr, my_col + dc),
            device_id_type=MESH,
        )

    def prepare():
        n = 32
        for lo in range(0, ROWS, n):
            rows, at = pl.ds(lo, n), pl.ds(TOP + lo, n)
            for p in range(2):
                cols = slice(p * LANES, (p + 1) * LANES)
                tap = tap_ref[rows, cols]
                for step in range(STEPS):
                    value = jnp.zeros(tap.shape, F32)
                    for which in range(NW):
                        value = jnp.where(tap == which, wave_ref[step, which], value)
                    load_ref[step, rows, cols] = value
                v = v_ref[p + 1, at, :]
                cap = cap_ref[rows, cols]
                held = mask_ref[rows, cols] == 1
                b = jnp.where(held, 0.0, cap)
                q = jnp.where(held, 0.0, cap * (load_ref[0, rows, cols] - shunt_ref[rows, cols] * v))
                b_ref[p + 1, at, :] = b
                q_ref[p + 1, at, :] = q
                part = {"b": b, "q": q}
                for comp in range(2):
                    c, r = c_ref[comp, p + 1, at, :], r_ref[comp, p + 1, at, :]
                    w = r * c
                    w_ref[comp, p + 1, at, :] = w
                    part["c%d" % comp], part["r%d" % comp], part["w%d" % comp] = c, r, w
                part["vh"] = v.astype(BF16).astype(F32)
                part["vl"] = v - part["vh"]
                lane = lane_of((n, LANES))
                for tile, names in enumerate(LANE_TILES):
                    mixed = None
                    for name, base in reversed(list(lane_slots(names))):
                        turned = roll(part[name], base if p == 0 else base + WIDTH[name])
                        mixed = turned if mixed is None else jnp.where(lane < base + WIDTH[name], turned, mixed)
                    sends_ref[p, rows, tile * LANES : (tile + 1) * LANES] = mixed.astype(BF16)

    def stack():
        for p in range(2):
            cols = slice(p * LANES, (p + 1) * LANES)
            for side in range(2):
                for name, width in SLOTS:
                    at = pl.ds(TOP if side == 0 else TOP + ROWS - width, width)
                    if name[0] == "v":
                        v = v_ref[p + 1, at, :]
                        value = v.astype(BF16).astype(F32)
                        value = value if name == "vh" else v - value
                    elif name in ("b", "q"):
                        value = (b_ref if name == "b" else q_ref)[p + 1, at, :]
                    else:
                        ref = {"w": w_ref, "c": c_ref, "r": r_ref}[name[0]]
                        value = ref[int(name[1]), p + 1, at, :]
                    stage_ref[side, pl.ds(ROW_BASE[name], width), cols] = value
        for side in range(2):
            for lo in range(0, 256, 64):
                sendv_ref[side, pl.ds(lo, 64), :] = stage_ref[side, pl.ds(lo, 64), :].astype(BF16)

    def put(name, tile, at, value):
        if name in ("b", "q"):
            (b_ref if name == "b" else q_ref)[tile, at, :] = value
        else:
            ref = {"w": w_ref, "c": c_ref, "r": r_ref}[name[0]]
            ref[int(name[1]), tile, at, :] = value

    def unpack_sides():
        n = 32
        for side in range(2):
            tile = 3 * side
            for lo in range(0, EXT, n):
                at = pl.ds(lo, n)
                got = {}
                for half, names in enumerate(LANE_TILES):
                    value = froms_ref[side, at, half * LANES : (half + 1) * LANES].astype(F32)
                    for name, base in lane_slots(names):
                        got[name] = roll(value, -(base + WIDTH[name]) if side == 0 else -base)
                v_ref[tile, at, :] = got["vh"] + got["vl"]
                for name in got:
                    if name[0] != "v":
                        put(name, tile, at, got[name])

    def unpack_ends():
        for side in range(2):
            for lo in range(0, 256, 64):
                stage_ref[side, pl.ds(lo, 64), :] = fromv_ref[side, pl.ds(lo, 64), :].astype(F32)
            for p in range(2):
                cols = slice(p * LANES, (p + 1) * LANES)
                for name, width in SLOTS:
                    at = pl.ds(TOP - width if side == 0 else TOP + ROWS, width)
                    value = stage_ref[side, pl.ds(ROW_BASE[name], width), cols]
                    if name == "vh":
                        v_ref[p + 1, at, :] = value + stage_ref[side, pl.ds(ROW_BASE["vl"], width), cols]
                    elif name != "vl":
                        put(name, p + 1, at, value)

    def drive(step):
        reach = WIDE if step == 0 else NEAR - 1
        lo = jnp.where(has_up, TOP - reach, TOP)
        hi = jnp.where(has_down, TOP + ROWS + reach - 1, TOP + ROWS)
        start, stop, n = (SKIP, EXT - SKIP, 16) if step == 0 else (FROM, EXT - FROM, 16)
        for base in range(start, stop, n):
            at, nxt, to = pl.ds(base, n), pl.ds(base + 1, n), pl.ds(base - SKIP, n)
            row = lax.broadcasted_iota(jnp.int32, (n, LANES), 0) + base
            lane = lane_of((n, LANES))
            inside = (row >= lo) & (row < hi)
            held = [inside & has_left, inside, inside, inside & has_right]
            v = [v_ref[k, at, :] for k in range(4)]
            for comp in range(2):
                out = []
                for k in range(4):
                    if step == 0:
                        w = w_ref[comp, k, at, :]
                    else:
                        w = r_ref[comp, k, at, :] * c_ref[comp, k, at, :]
                    if comp == 0:
                        beside = v_ref[k, nxt, :]
                    else:
                        beside = roll(jnp.where(lane == 0, v[min(k + 1, 3)], v[k]), LANES - 1)
                    out.append(jnp.where(held[k], v[k] - beside - w, 0.0))
                tl, ta, tb, tr = out
                slot = 6 * comp
                if step == 0 or comp == 1:
                    drive_ref[slot, to, :] = roll(jnp.where(lane < 64, ta, tl), 64)
                drive_ref[slot + 1, to, :] = jnp.where(lane < 96, ta, tl)
                drive_ref[slot + 2, to, :] = roll(jnp.where(lane < 32, tb, ta), 64)
                drive_ref[slot + 3, to, :] = jnp.where(lane < 96, tb, ta)
                drive_ref[slot + 4, to, :] = roll(jnp.where(lane < 32, tr, tb), 64)
                if step == 0:
                    drive_ref[slot + 5, to, :] = jnp.where(lane < 96, tr, tb)

    def convolve(step, comp):
        if step == 0:
            blocks, start, n, to = (-1, 0, 1, 2, 3, 4), 4, 48, 4
        elif comp == 0:
            blocks, start, n, to = (0, 1, 2, 3), 20, 40, 20
        else:
            blocks, start, n, to = (-1, 0, 1, 2, 3), 24, 32, 24
        total = n * len(blocks)
        for tap in range(TAPS):
            pieces = [drive_ref[6 * comp + 1 + k, pl.ds(start + tap, n, stride=GROUP), :] for k in blocks]
            lhs_ref[0:total, tap * LANES : (tap + 1) * LANES] = jnp.concatenate(pieces, axis=0).astype(BF16)
        product = jnp.dot(lhs_ref[0:total, :], table_ref[comp], preferred_element_type=F32)
        low = lane_of((n, LANES)) < 64
        for t in range(GROUP):
            half = product[:, (t // 2) * LANES : (t // 2 + 1) * LANES]
            part = {k: half[i * n : (i + 1) * n] for i, k in enumerate(blocks)}
            for tile, (even, odd) in enumerate(((None, -1), (0, 1), (2, 3), (4, None))):
                if even not in part and odd not in part:
                    continue
                if even is None:
                    value = roll(part[odd], 64) if t % 2 == 0 else part[odd]
                elif odd is None:
                    value = part[even] if t % 2 == 0 else roll(part[even], 64)
                elif t % 2 == 0:
                    value = jnp.where(low, part[even], roll(part[odd], 64))
                else:
                    value = jnp.where(low, roll(part[even], 64), part[odd])
                flow_ref[comp, tile, pl.ds(to + t, n, stride=GROUP), :] = value

    def advance_frame():
        n = 16
        lo = jnp.where(has_up, 0, TOP)
        hi = jnp.where(has_down, EXT, TOP + ROWS)
        for base in range(FROM, EXT - FROM, n):
            at, flow = pl.ds(base, n), pl.ds(base - FROM, n)
            row = lax.broadcasted_iota(jnp.int32, (n, LANES), 0) + base
            inside = (row >= lo) & (row < hi)
            held = [inside & has_left, inside, inside, inside & has_right]
            for comp in range(2):
                for k in range(4):
                    value = c_ref[comp, k, at, :] + flow_ref[comp, k, flow, :]
                    c_ref[comp, k, at, :] = jnp.where(held[k], value, 0.0)

    def divergence(base, n, k):
        at = pl.ds(base, n)
        lane = lane_of((n, LANES))
        c1 = c_ref[1, k, at, :]
        before_x = c_ref[0, k, pl.ds(base - 1, n), :]
        before_y = roll(jnp.where(lane == LANES - 1, c_ref[1, max(k - 1, 0), at, :], c1), 1)
        return c_ref[0, k, at, :] - before_x + c1 - before_y

    def update_frame():
        n = 16
        for base in range(FROM, EXT - FROM, n):
            at = pl.ds(base, n)
            for k in range(4):
                b = b_ref[k, at, :]
                value = v_ref[k, at, :] + q_ref[k, at, :] - b * divergence(base, n, k)
                v_ref[k, at, :] = jnp.where(b == 0.0, 0.0, value)

    def finish():
        n = 32
        for k in range(1, 3):
            at = pl.ds(TOP - 8, 8)
            head = c_ref[0, k, at, :] + flow_ref[0, k, pl.ds(TOP - 8 - FROM, 8), :]
            c_ref[0, k, at, :] = jnp.where(has_up, head, 0.0)
        for lo in range(0, ROWS, n):
            at, flow = pl.ds(TOP + lo, n), pl.ds(TOP + lo - FROM, n)
            left = c_ref[1, 0, at, :] + flow_ref[1, 0, flow, :]
            c_ref[1, 0, at, :] = jnp.where(has_left, left, 0.0)
            for k in range(1, 3):
                cols = slice((k - 1) * LANES, k * LANES)
                for comp in range(2):
                    value = c_ref[comp, k, at, :] + flow_ref[comp, k, flow, :]
                    c_ref[comp, k, at, :] = value
                    cout_ref[comp, pl.ds(lo, n), cols] = value
        for lo in range(0, ROWS, n):
            at, rows = pl.ds(TOP + lo, n), pl.ds(lo, n)
            for k in range(1, 3):
                cols = slice((k - 1) * LANES, k * LANES)
                v = v_ref[k, at, :]
                change = load_ref[1, rows, cols] - divergence(TOP + lo, n, k) - shunt_ref[rows, cols] * v
                vout_ref[rows, cols] = jnp.where(mask_ref[rows, cols] == 1, 0.0, v + cap_ref[rows, cols] * change)

    for one in loads:
        one.wait()
    prepare()
    stack()
    pl.semaphore_wait(barrier, (1 + one_if(has_up) + one_if(has_down)) * (1 + one_if(has_left) + one_if(has_right)) - 1)
    for which, (dr, dc) in enumerate(DIRECTIONS):
        @pl.when(exists(dr, dc))
        def _(which=which):
            message(which).start()
    build_table(k_ref, 0, pad_ref, base_ref, table_ref)
    build_table(k_ref, 1, pad_ref, base_ref, table_ref)
    for which, (dr, dc) in enumerate(DIRECTIONS):
        @pl.when(exists(-dr, -dc))
        def _(which=which):
            message(which).wait_recv()
    unpack_sides()
    unpack_ends()
    drive(0)
    convolve(0, 0)
    convolve(0, 1)
    advance_frame()
    update_frame()
    drive(1)
    convolve(1, 0)
    convolve(1, 1)
    finish()
    for which, (dr, dc) in enumerate(DIRECTIONS):
        @pl.when(exists(dr, dc))
        def _(which=which):
            message(which).wait_send()


def local(voltage, currents, resistance, inverse_cap, shunt_conductance, tap_index, pad_mask, waveforms, k_window):
    hbm = pl.BlockSpec(memory_space=pltpu.HBM)
    vmem = pl.BlockSpec(memory_space=pltpu.VMEM)
    block = (ROWS, COLS)
    frame = (4, EXT, LANES)
    scratch = [
        pltpu.VMEM(block, F32),
        pltpu.VMEM(block, F32),
        pltpu.VMEM(block, jnp.int32),
        pltpu.VMEM(block, jnp.int32),
        pltpu.VMEM(frame, F32),
        pltpu.VMEM((2, *frame), F32),
        pltpu.VMEM((2, *frame), F32),
        pltpu.VMEM((2, *frame), F32),
        pltpu.VMEM(frame, F32),
        pltpu.VMEM(frame, F32),
        pltpu.VMEM((2, 256, COLS), F32),
        pltpu.VMEM((2, 256, COLS), BF16),
        pltpu.VMEM((2, ROWS, COLS), BF16),
        pltpu.VMEM((2, 256, COLS), BF16),
        pltpu.VMEM((2, EXT, COLS), BF16),
        pltpu.VMEM((12, DEEP, LANES), F32),
        pltpu.VMEM((288, DEPTH), BF16),
        pltpu.VMEM((2, DEPTH, 2 * LANES), BF16),
        pltpu.VMEM((48, LANES), F32),
        pltpu.VMEM((40, LANES), F32),
        pltpu.VMEM((STEPS, *block), F32),
        pltpu.VMEM((2, 4, FLOW, LANES), F32),
        pltpu.SMEM((STEPS, NW), F32),
        pltpu.VMEM((SPAN, 2, SPAN), BF16),
        pltpu.SemaphoreType.DMA((16,)),
        pltpu.SemaphoreType.DMA((8,)),
        pltpu.SemaphoreType.DMA((8,)),
    ]
    call = pl.pallas_call(
        kernel,
        out_shape=(jax.ShapeDtypeStruct(block, F32), jax.ShapeDtypeStruct((2, *block), F32)),
        in_specs=[hbm] * 9,
        out_specs=(vmem, vmem),
        scratch_shapes=scratch,
        compiler_params=pltpu.CompilerParams(
            collective_id=0, has_side_effects=True, vmem_limit_bytes=40 * 1024 * 1024
        ),
    )
    held = [waveforms, jnp.transpose(k_window, (1, 0, 2)), voltage, currents, resistance, inverse_cap]
    held += [shunt_conductance, tap_index, pad_mask]
    held = [pltpu.with_memory_space_constraint(one, pltpu.HBM) for one in held]
    return call(*held)


def solution(mesh):
    placed = (
        P("row", "col"),
        P(None, "row", "col"),
        P(None, "row", "col"),
        P("row", "col"),
        P("row", "col"),
        P("row", "col"),
        P("row", "col"),
        P(),
        P(),
    )
    return jax.shard_map(
        local,
        mesh=mesh,
        in_specs=placed,
        out_specs=(P("row", "col"), P(None, "row", "col")),
        check_vma=False,
    )
```

```python
import functools

import jax
import jax.numpy as jnp
from jax import lax
from jax.experimental import pallas as pl
from jax.experimental.pallas import tpu as pltpu
from jax.sharding import PartitionSpec as P

HALF = 16
SPAN = 2 * HALF + 1
STEPS = 2
NW = 8
ROWS = 128
COLS = 256
LANES = 128
TOP = 48
EXT = ROWS + 2 * TOP
SKIP = 8
PITCH = 33
WIDE = 34
NEAR = 18
FLOW = 27
FROM = 24
GROUP = 8
STRIP = LANES // 4
TAPS = SPAN + GROUP - 1
CHUNKS = TAPS // 2
DEPTH = CHUNKS * LANES
BLOCKS = CHUNKS - 2
MESH = pl.DeviceIdType.MESH
F32 = jnp.float32
BF16 = jnp.bfloat16
DIRECTIONS = ((-1, 0), (1, 0), (0, -1), (0, 1), (-1, -1), (-1, 1), (1, -1), (1, 1))


def lane_of(shape):
    return lax.broadcasted_iota(jnp.int32, shape, len(shape) - 1)


def roll(value, amount):
    return pltpu.roll(value, amount % LANES, 1)


def one_if(flag):
    return jnp.where(flag, 1, 0)


def build_table(k_ref, pad_ref, base_ref, table_ref):
    tap = lax.broadcasted_iota(jnp.int32, (LANES, LANES), 0)
    lane = lax.broadcasted_iota(jnp.int32, (LANES, LANES), 1)
    for comp in range(2):
        pad_ref[comp] = jnp.zeros(pad_ref.shape[1:], F32)
        pad_ref[comp, 8 : 8 + SPAN, 0:SPAN] = k_ref[:, comp, :].astype(F32)
        for kind in range(2):
            total = None
            for t in range(4):
                hit = (((STRIP * t + HALF - tap) & 127) == lane) & (tap >= kind) & (tap < SPAN - 1 + kind)
                rows = pad_ref[comp, 8 - t : 48 - t, :].astype(BF16)
                part = jnp.dot(rows, jnp.where(hit, 1.0, 0.0).astype(BF16), preferred_element_type=F32)
                total = part if total is None else total + part
            base_ref[comp, kind] = total
    within = lax.broadcasted_iota(jnp.int32, (64, LANES), 0)
    strip = lax.broadcasted_iota(jnp.int32, (64, LANES), 1) & (STRIP - 1)
    inside = ((within - strip + HALF) & 63) < SPAN

    def turned(row, count, shift):
        return pltpu.roll(jnp.broadcast_to(row, (count, LANES)), shift, 1, stride=1, stride_axis=0)

    def one(index, carry):
        for comp in range(2):
            halves = []
            for odd in range(2):
                near = base_ref[comp, 0, pl.ds(2 * index + odd, 1), :]
                far = base_ref[comp, 1, pl.ds(2 * index + odd, 1), :]
                whole = [turned(near, 16, 0), turned(far, 32, 16), turned(near, 16, LANES - 16)]
                halves.append(jnp.where(inside, jnp.concatenate(whole, axis=0), 0.0))
            block = jnp.concatenate(halves, axis=0).astype(BF16)
            table_ref[comp, pl.ds(pl.multiple_of(index * LANES, LANES), LANES), 0:LANES] = block
            table_ref[comp, pl.ds(pl.multiple_of((index + 2) * LANES, LANES), LANES), LANES:] = block
        return carry

    lax.fori_loop(0, BLOCKS, one, 0, unroll=2)
    blank = jnp.zeros((2 * LANES, LANES), BF16)
    for comp in range(2):
        table_ref[comp, BLOCKS * LANES :, 0:LANES] = blank
        table_ref[comp, 0 : 2 * LANES, LANES:] = blank


SLOTS = (("vh", WIDE), ("vl", WIDE), ("w0", WIDE), ("w1", WIDE), ("c0", NEAR), ("c1", NEAR), ("r0", NEAR), ("r1", NEAR), ("b", NEAR), ("q", NEAR))
ROW_BASE = {name: sum(width for _, width in SLOTS[:i]) for i, (name, _) in enumerate(SLOTS)}
WIDTH = dict(SLOTS)
LANE_TILES = (("vh", "vl", "w0", "q"), ("w1", "c0", "c1", "r0", "r1", "b"))


def lane_slots(names):
    base = 0
    for name in names:
        yield name, base
        base += WIDTH[name]


def kernel(
    wave_hbm, k_hbm, v_hbm, c_hbm, r_hbm, cap_hbm, shunt_hbm, tap_hbm, mask_hbm,
    vout_ref, cout_ref,
    cap_ref, shunt_ref, tap_ref, mask_ref,
    v_ref, w_ref, c_ref, r_ref, b_ref, q_ref,
    stage_ref, sendv_ref, sends_ref, fromv_ref, froms_ref,
    drive_ref, table_ref, pad_ref, base_ref, load_ref, flow_ref,
    wave_ref, k_ref, load_sem, send_sem, recv_sem,
):
    my_row, my_col = lax.axis_index("row"), lax.axis_index("col")
    n_row, n_col = lax.axis_size("row"), lax.axis_size("col")

    def exists(dr, dc):
        row, col = my_row + dr, my_col + dc
        ok = None
        for spot, count, delta in ((row, n_row, dr), (col, n_col, dc)):
            if delta:
                here = (spot >= 0) & (spot < count)
                ok = here if ok is None else ok & here
        return ok

    own = pl.ds(TOP, ROWS)
    pairs = [(k_hbm, k_ref), (wave_hbm, wave_ref)]
    pairs += [(cap_hbm, cap_ref), (shunt_hbm, shunt_ref), (tap_hbm, tap_ref), (mask_hbm, mask_ref)]
    for p in range(2):
        cols = pl.ds(p * LANES, LANES)
        pairs.append((v_hbm.at[:, cols], v_ref.at[p + 1, own, :]))
        for comp in range(2):
            pairs.append((c_hbm.at[comp, :, cols], c_ref.at[comp, p + 1, own, :]))
            pairs.append((r_hbm.at[comp, :, cols], r_ref.at[comp, p + 1, own, :]))
    loads = [pltpu.make_async_copy(src, dst, load_sem.at[i]) for i, (src, dst) in enumerate(pairs)]
    for one in loads:
        one.start()
    barrier = pltpu.get_barrier_semaphore()
    for dr, dc in DIRECTIONS:
        @pl.when(exists(dr, dc))
        def _(dr=dr, dc=dc):
            pl.semaphore_signal(barrier, inc=1, device_id=(my_row + dr, my_col + dc), device_id_type=MESH)

    has_up, has_down, has_left, has_right = (exists(*d) for d in DIRECTIONS[:4])

    for side, missing in enumerate((has_up, has_down)):
        @pl.when(jnp.logical_not(missing))
        def _(side=side):
            fromv_ref[side] = jnp.zeros(fromv_ref.shape[1:], BF16)
            rows = pl.ds(0, TOP) if side == 0 else pl.ds(TOP + ROWS, TOP)
            for other in range(2):
                froms_ref[other, rows, :] = jnp.zeros((TOP, COLS), BF16)

    for side, missing in enumerate((has_left, has_right)):
        @pl.when(jnp.logical_not(missing))
        def _(side=side):
            froms_ref[side] = jnp.zeros(froms_ref.shape[1:], BF16)

    def message(which):
        dr, dc = DIRECTIONS[which]
        low, mid, high = pl.ds(0, TOP), pl.ds(TOP, ROWS), pl.ds(TOP + ROWS, TOP)
        first, last = pl.ds(0, TOP), pl.ds(ROWS - TOP, TOP)
        if dc == 0:
            side = 0 if dr > 0 else 1
            source, target = sendv_ref.at[1 - side], fromv_ref.at[side]
        else:
            side = 0 if dc > 0 else 1
            out, land = sends_ref.at[1 - side], froms_ref.at[side]
            source = out if dr == 0 else out.at[first if dr < 0 else last, :]
            target = land.at[mid if dr == 0 else (high if dr < 0 else low), :]
        return pltpu.make_async_remote_copy(
            src_ref=source,
            dst_ref=target,
            send_sem=send_sem.at[which],
            recv_sem=recv_sem.at[which],
            device_id=(my_row + dr, my_col + dc),
            device_id_type=MESH,
        )

    def prepare():
        n = 32
        for lo in range(0, ROWS, n):
            rows, at = pl.ds(lo, n), pl.ds(TOP + lo, n)
            for p in range(2):
                cols = slice(p * LANES, (p + 1) * LANES)
                tap = tap_ref[rows, cols]
                for step in range(STEPS):
                    value = jnp.zeros(tap.shape, F32)
                    for which in range(NW):
                        value = jnp.where(tap == which, wave_ref[step, which], value)
                    load_ref[step, rows, cols] = value
                v = v_ref[p + 1, at, :]
                cap = cap_ref[rows, cols]
                held = mask_ref[rows, cols] == 1
                b = jnp.where(held, 0.0, cap)
                q = jnp.where(held, 0.0, cap * (load_ref[0, rows, cols] - shunt_ref[rows, cols] * v))
                b_ref[p + 1, at, :] = b
                q_ref[p + 1, at, :] = q
                part = {"b": b, "q": q}
                for comp in range(2):
                    c, r = c_ref[comp, p + 1, at, :], r_ref[comp, p + 1, at, :]
                    w = r * c
                    w_ref[comp, p + 1, at, :] = w
                    part["c%d" % comp], part["r%d" % comp], part["w%d" % comp] = c, r, w
                part["vh"] = v.astype(BF16).astype(F32)
                part["vl"] = v - part["vh"]
                lane = lane_of((n, LANES))
                for tile, names in enumerate(LANE_TILES):
                    mixed = None
                    for name, base in reversed(list(lane_slots(names))):
                        turned = roll(part[name], base if p == 0 else base + WIDTH[name])
                        mixed = turned if mixed is None else jnp.where(lane < base + WIDTH[name], turned, mixed)
                    sends_ref[p, rows, tile * LANES : (tile + 1) * LANES] = mixed.astype(BF16)

    def stack():
        for p in range(2):
            cols = slice(p * LANES, (p + 1) * LANES)
            for side in range(2):
                for name, width in SLOTS:
                    at = pl.ds(TOP if side == 0 else TOP + ROWS - width, width)
                    if name[0] == "v":
                        v = v_ref[p + 1, at, :]
                        value = v.astype(BF16).astype(F32)
                        value = value if name == "vh" else v - value
                    elif name in ("b", "q"):
                        value = (b_ref if name == "b" else q_ref)[p + 1, at, :]
                    else:
                        ref = {"w": w_ref, "c": c_ref, "r": r_ref}[name[0]]
                        value = ref[int(name[1]), p + 1, at, :]
                    stage_ref[side, pl.ds(ROW_BASE[name], width), cols] = value
        for side in range(2):
            for lo in range(0, 256, 64):
                sendv_ref[side, pl.ds(lo, 64), :] = stage_ref[side, pl.ds(lo, 64), :].astype(BF16)

    def put(name, tile, at, value):
        if name in ("b", "q"):
            (b_ref if name == "b" else q_ref)[tile, at, :] = value
        else:
            ref = {"w": w_ref, "c": c_ref, "r": r_ref}[name[0]]
            ref[int(name[1]), tile, at, :] = value

    def unpack_sides():
        n = 32
        for side in range(2):
            tile = 3 * side
            for lo in range(0, EXT, n):
                at = pl.ds(lo, n)
                got = {}
                for half, names in enumerate(LANE_TILES):
                    value = froms_ref[side, at, half * LANES : (half + 1) * LANES].astype(F32)
                    for name, base in lane_slots(names):
                        got[name] = roll(value, -(base + WIDTH[name]) if side == 0 else -base)
                v_ref[tile, at, :] = got["vh"] + got["vl"]
                for name in got:
                    if name[0] != "v":
                        put(name, tile, at, got[name])

    def unpack_ends():
        for side in range(2):
            for lo in range(0, 256, 64):
                stage_ref[side, pl.ds(lo, 64), :] = fromv_ref[side, pl.ds(lo, 64), :].astype(F32)
            for p in range(2):
                cols = slice(p * LANES, (p + 1) * LANES)
                for name, width in SLOTS:
                    at = pl.ds(TOP - width if side == 0 else TOP + ROWS, width)
                    value = stage_ref[side, pl.ds(ROW_BASE[name], width), cols]
                    if name == "vh":
                        v_ref[p + 1, at, :] = value + stage_ref[side, pl.ds(ROW_BASE["vl"], width), cols]
                    elif name != "vl":
                        put(name, p + 1, at, value)

    def windows(tiles, nexts, wanted):
        lane = lane_of(tiles[0].shape)
        mark, low = lane & 63, lane < 64
        pair = {}
        for at in range(4):
            if at > 0:
                pair[2 * at - 2] = jnp.where(low, tiles[at], roll(nexts[at], 64))
            if at < 3:
                pair[2 * at - 1] = jnp.where(low, roll(tiles[at], 64), nexts[at])
        out = {}
        for k in wanted:
            i = k // 2
            if k % 2 == 0:
                out[k] = jnp.where(mark < 48, pair[i], pair[i - 1])
            else:
                out[k] = jnp.where(mark < 16, pair[i + 1], pair[i])
        return out

    def drive(step, comp):
        reach = WIDE if step == 0 else NEAR - 1
        lo = jnp.where(has_up, TOP - reach, TOP)
        hi = jnp.where(has_down, TOP + ROWS + reach - 1, TOP + ROWS)
        start, stop, n = (SKIP, EXT - SKIP, 16) if step == 0 else (FROM, EXT - FROM, 16)
        carried = {}
        for base in reversed(range(start, stop, n)):
            at, nxt = pl.ds(base, n), pl.ds(base + 1, n)
            row = lax.broadcasted_iota(jnp.int32, (n, LANES), 0) + base
            lane = lane_of((n, LANES))
            inside = (row >= lo) & (row < hi)
            held = [inside & has_left, inside, inside, inside & has_right]
            v = [v_ref[k, at, :] for k in range(4)]
            if True:
                out = []
                for k in range(4):
                    if step == 0:
                        w = w_ref[comp, k, at, :]
                    else:
                        w = r_ref[comp, k, at, :] * c_ref[comp, k, at, :]
                    if comp == 0:
                        beside = v_ref[k, nxt, :]
                    else:
                        beside = roll(jnp.where(lane == 0, v[min(k + 1, 3)], v[k]), LANES - 1)
                    out.append(jnp.where(held[k], v[k] - beside - w, 0.0))
                nexts = []
                for k in range(4):
                    after = carried.get((comp, k), out[k][0:8])
                    nexts.append(pltpu.roll(jnp.concatenate([out[k], after], axis=0), n + 7, 0)[0:n])
                    carried[comp, k] = out[k][0:8]
                for k, value in windows(out, nexts, blocks_of(step, comp)).items():
                    for g in range(n // 8):
                        spot = pl.ds((base - SKIP) // 8 + g, 8, stride=PITCH)
                        drive_ref[10 * comp + k + 1, spot, :] = value[8 * g : 8 * g + 8]

    def blocks_of(step, comp):
        if step == 0:
            return tuple(range(-1, 9))
        return tuple(range(0, 8)) if comp == 0 else tuple(range(-1, 8))

    def convolve(step, comp):
        blocks = blocks_of(step, comp)
        start, n = (0, 24) if step == 0 else ((16, 24) if comp == 0 else (24, 16))
        part = [{}, {}]
        for odd in range(2):
            mine = [k for k in blocks if k % 2 == odd]
            columns = []
            for chunk in range(CHUNKS):
                group, phase = divmod(2 * chunk, 8)
                at = pl.ds(phase * PITCH + start // 8 + group, n)
                columns.append(jnp.concatenate([drive_ref[10 * comp + 1 + k, at, :] for k in mine], axis=0).astype(BF16))
            if odd:
                order = [(i ^ 1) * 32 for i in range(DEPTH // 32)]
                weights = jnp.concatenate([table_ref[comp, lo : lo + 32, :] for lo in order], axis=0)
            else:
                weights = table_ref[comp]
            product = jnp.dot(jnp.concatenate(columns, axis=1), weights, preferred_element_type=F32)
            for i, k in enumerate(mine):
                for side in range(2):
                    part[side][k] = product[i * n : (i + 1) * n, side * LANES : (side + 1) * LANES]
        lane = lane_of((n, LANES))
        for side in range(2):
            for t in range(4):
                for tile in range(4):
                    value = None
                    for q in reversed(range(4)):
                        k = 4 * (tile - 1) + q
                        if k in part[side]:
                            turn = (q - t) % 4
                            piece = roll(part[side][k], STRIP * turn) if turn else part[side][k]
                            value = piece if value is None else jnp.where(lane < STRIP * (q + 1), piece, value)
                    if value is not None:
                        flow_ref[comp, tile, pl.ds((4 * side + t) * FLOW + start // 8, n), :] = value

    def flow(comp, tile, first, n):
        parts = [flow_ref[comp, tile, pl.ds(first // 8 + g, 8, stride=FLOW), :] for g in range(n // 8)]
        return jnp.concatenate(parts, axis=0) if len(parts) > 1 else parts[0]

    def advance_frame():
        n = 16
        lo = jnp.where(has_up, 0, TOP)
        hi = jnp.where(has_down, EXT, TOP + ROWS)
        for base in range(FROM, EXT - FROM, n):
            at = pl.ds(base, n)
            row = lax.broadcasted_iota(jnp.int32, (n, LANES), 0) + base
            inside = (row >= lo) & (row < hi)
            held = [inside & has_left, inside, inside, inside & has_right]
            for comp in range(2):
                for k in range(4):
                    value = c_ref[comp, k, at, :] + flow(comp, k, base - FROM, n)
                    c_ref[comp, k, at, :] = jnp.where(held[k], value, 0.0)

    def divergence(base, n, k):
        at = pl.ds(base, n)
        lane = lane_of((n, LANES))
        c1 = c_ref[1, k, at, :]
        before_x = c_ref[0, k, pl.ds(base - 1, n), :]
        before_y = roll(jnp.where(lane == LANES - 1, c_ref[1, max(k - 1, 0), at, :], c1), 1)
        return c_ref[0, k, at, :] - before_x + c1 - before_y

    def update_frame():
        n = 16
        for base in range(FROM, EXT - FROM, n):
            at = pl.ds(base, n)
            for k in range(4):
                b = b_ref[k, at, :]
                value = v_ref[k, at, :] + q_ref[k, at, :] - b * divergence(base, n, k)
                v_ref[k, at, :] = jnp.where(b == 0.0, 0.0, value)

    def finish():
        n = 32
        for k in range(1, 3):
            at = pl.ds(TOP - 8, 8)
            head = c_ref[0, k, at, :] + flow(0, k, TOP - 8 - FROM, 8)
            c_ref[0, k, at, :] = jnp.where(has_up, head, 0.0)
        for lo in range(0, ROWS, n):
            at, first = pl.ds(TOP + lo, n), TOP + lo - FROM
            left = c_ref[1, 0, at, :] + flow(1, 0, first, n)
            c_ref[1, 0, at, :] = jnp.where(has_left, left, 0.0)
            for k in range(1, 3):
                cols = slice((k - 1) * LANES, k * LANES)
                for comp in range(2):
                    value = c_ref[comp, k, at, :] + flow(comp, k, first, n)
                    c_ref[comp, k, at, :] = value
                    cout_ref[comp, pl.ds(lo, n), cols] = value
        for lo in range(0, ROWS, n):
            at, rows = pl.ds(TOP + lo, n), pl.ds(lo, n)
            for k in range(1, 3):
                cols = slice((k - 1) * LANES, k * LANES)
                v = v_ref[k, at, :]
                change = load_ref[1, rows, cols] - divergence(TOP + lo, n, k) - shunt_ref[rows, cols] * v
                vout_ref[rows, cols] = jnp.where(mask_ref[rows, cols] == 1, 0.0, v + cap_ref[rows, cols] * change)

    for one in loads:
        one.wait()
    prepare()
    stack()
    pl.semaphore_wait(barrier, (1 + one_if(has_up) + one_if(has_down)) * (1 + one_if(has_left) + one_if(has_right)) - 1)
    for which, (dr, dc) in enumerate(DIRECTIONS):
        @pl.when(exists(dr, dc))
        def _(which=which):
            message(which).start()
    build_table(k_ref, pad_ref, base_ref, table_ref)
    for which, (dr, dc) in enumerate(DIRECTIONS):
        @pl.when(exists(-dr, -dc))
        def _(which=which):
            message(which).wait_recv()
    unpack_sides()
    unpack_ends()
    for comp in range(2):
        drive(0, comp)
        convolve(0, comp)
    advance_frame()
    update_frame()
    for comp in range(2):
        drive(1, comp)
        convolve(1, comp)
    finish()
    for which, (dr, dc) in enumerate(DIRECTIONS):
        @pl.when(exists(dr, dc))
        def _(which=which):
            message(which).wait_send()


def local(voltage, currents, resistance, inverse_cap, shunt_conductance, tap_index, pad_mask, waveforms, k_window):
    hbm = pl.BlockSpec(memory_space=pltpu.HBM)
    vmem = pl.BlockSpec(memory_space=pltpu.VMEM)
    block = (ROWS, COLS)
    frame = (4, EXT, LANES)
    scratch = [
        pltpu.VMEM(block, F32),
        pltpu.VMEM(block, F32),
        pltpu.VMEM(block, jnp.int32),
        pltpu.VMEM(block, jnp.int32),
        pltpu.VMEM(frame, F32),
        pltpu.VMEM((2, *frame), F32),
        pltpu.VMEM((2, *frame), F32),
        pltpu.VMEM((2, *frame), F32),
        pltpu.VMEM(frame, F32),
        pltpu.VMEM(frame, F32),
        pltpu.VMEM((2, 256, COLS), F32),
        pltpu.VMEM((2, 256, COLS), BF16),
        pltpu.VMEM((2, ROWS, COLS), BF16),
        pltpu.VMEM((2, 256, COLS), BF16),
        pltpu.VMEM((2, EXT, COLS), BF16),
        pltpu.VMEM((20, 8 * PITCH, LANES), F32),
        pltpu.VMEM((2, DEPTH, 2 * LANES), BF16),
        pltpu.VMEM((2, 48, LANES), F32),
        pltpu.VMEM((2, 2, 40, LANES), F32),
        pltpu.VMEM((STEPS, *block), F32),
        pltpu.VMEM((2, 4, 8 * FLOW, LANES), F32),
        pltpu.SMEM((STEPS, NW), F32),
        pltpu.VMEM((SPAN, 2, SPAN), BF16),
        pltpu.SemaphoreType.DMA((16,)),
        pltpu.SemaphoreType.DMA((8,)),
        pltpu.SemaphoreType.DMA((8,)),
    ]
    call = pl.pallas_call(
        kernel,
        out_shape=(jax.ShapeDtypeStruct(block, F32), jax.ShapeDtypeStruct((2, *block), F32)),
        in_specs=[hbm] * 9,
        out_specs=(vmem, vmem),
        scratch_shapes=scratch,
        compiler_params=pltpu.CompilerParams(
            collective_id=0, has_side_effects=True, vmem_limit_bytes=40 * 1024 * 1024
        ),
    )
    held = [waveforms, jnp.transpose(k_window, (1, 0, 2)), voltage, currents, resistance, inverse_cap]
    held += [shunt_conductance, tap_index, pad_mask]
    held = [pltpu.with_memory_space_constraint(one, pltpu.HBM) for one in held]
    return call(*held)


def solution(mesh):
    placed = (
        P("row", "col"),
        P(None, "row", "col"),
        P(None, "row", "col"),
        P("row", "col"),
        P("row", "col"),
        P("row", "col"),
        P("row", "col"),
        P(),
        P(),
    )
    return jax.shard_map(
        local,
        mesh=mesh,
        in_specs=placed,
        out_specs=(P("row", "col"), P(None, "row", "col")),
        check_vma=False,
    )
```

```python
import functools

import jax
import jax.numpy as jnp
from jax import lax
from jax.experimental import pallas as pl
from jax.experimental.pallas import tpu as pltpu
from jax.sharding import PartitionSpec as P

HALF = 16
SPAN = 2 * HALF + 1
STEPS = 2
NW = 8
ROWS = 128
COLS = 256
LANES = 128
TOP = 48
EXT = ROWS + 2 * TOP
SKIP = 8
PITCH = 33
WIDE = 34
NEAR = 18
FLOW = 27
FROM = 24
GROUP = 8
STRIP = LANES // 4
TAPS = SPAN + GROUP - 1
CHUNKS = TAPS // 2
DEPTH = CHUNKS * LANES
BLOCKS = CHUNKS - 2
MESH = pl.DeviceIdType.MESH
F32 = jnp.float32
BF16 = jnp.bfloat16
DIRECTIONS = ((-1, 0), (1, 0), (0, -1), (0, 1), (-1, -1), (-1, 1), (1, -1), (1, 1))


def lane_of(shape):
    return lax.broadcasted_iota(jnp.int32, shape, len(shape) - 1)


def roll(value, amount):
    return pltpu.roll(value, amount % LANES, 1)


def one_if(flag):
    return jnp.where(flag, 1, 0)


def build_table(k_ref, pad_ref, base_ref, table_ref):
    tap = lax.broadcasted_iota(jnp.int32, (LANES, LANES), 0)
    lane = lax.broadcasted_iota(jnp.int32, (LANES, LANES), 1)
    for comp in range(2):
        pad_ref[comp] = jnp.zeros(pad_ref.shape[1:], F32)
        pad_ref[comp, 8 : 8 + SPAN, 0:SPAN] = k_ref[:, comp, :].astype(F32)
        for kind in range(2):
            total = None
            for t in range(4):
                hit = (((STRIP * t + HALF - tap) & 127) == lane) & (tap >= kind) & (tap < SPAN - 1 + kind)
                rows = pad_ref[comp, 8 - t : 48 - t, :].astype(BF16)
                part = jnp.dot(rows, jnp.where(hit, 1.0, 0.0).astype(BF16), preferred_element_type=F32)
                total = part if total is None else total + part
            base_ref[comp, kind] = total
    within = lax.broadcasted_iota(jnp.int32, (64, LANES), 0)
    strip = lax.broadcasted_iota(jnp.int32, (64, LANES), 1) & (STRIP - 1)
    inside = ((within - strip + HALF) & 63) < SPAN

    def turned(row, count, shift):
        return pltpu.roll(jnp.broadcast_to(row, (count, LANES)), shift, 1, stride=1, stride_axis=0)

    def one(index, carry):
        for comp in range(2):
            halves = []
            for odd in range(2):
                near = base_ref[comp, 0, pl.ds(2 * index + odd, 1), :]
                far = base_ref[comp, 1, pl.ds(2 * index + odd, 1), :]
                whole = [turned(near, 16, 0), turned(far, 32, 16), turned(near, 16, LANES - 16)]
                halves.append(jnp.where(inside, jnp.concatenate(whole, axis=0), 0.0))
            block = jnp.concatenate(halves, axis=0).astype(BF16)
            table_ref[comp, pl.ds(pl.multiple_of(index * LANES, LANES), LANES), 0:LANES] = block
            table_ref[comp, pl.ds(pl.multiple_of((index + 2) * LANES, LANES), LANES), LANES:] = block
        return carry

    lax.fori_loop(0, BLOCKS, one, 0, unroll=2)
    blank = jnp.zeros((2 * LANES, LANES), BF16)
    for comp in range(2):
        table_ref[comp, BLOCKS * LANES :, 0:LANES] = blank
        table_ref[comp, 0 : 2 * LANES, LANES:] = blank


SLOTS = (("vh", WIDE), ("vl", WIDE), ("w0", WIDE), ("w1", WIDE), ("c0", NEAR), ("c1", NEAR), ("r0", NEAR), ("r1", NEAR), ("b", NEAR), ("q", NEAR))
ROW_BASE = {name: sum(width for _, width in SLOTS[:i]) for i, (name, _) in enumerate(SLOTS)}
WIDTH = dict(SLOTS)
LANE_TILES = (("vh", "vl", "w0", "q"), ("w1", "c0", "c1", "r0", "r1", "b"))


def lane_slots(names):
    base = 0
    for name in names:
        yield name, base
        base += WIDTH[name]


def kernel(
    wave_hbm, k_hbm, v_hbm, c_hbm, r_hbm, cap_hbm, shunt_hbm, tap_hbm, mask_hbm,
    vout_ref, cout_ref,
    cap_ref, shunt_ref, tap_ref, mask_ref,
    v_ref, w_ref, c_ref, r_ref, b_ref, q_ref,
    stage_ref, sendv_ref, sends_ref, fromv_ref, froms_ref,
    drive_ref, table_ref, pad_ref, base_ref, load_ref, flow_ref,
    wave_ref, k_ref, load_sem, send_sem, recv_sem,
):
    my_row, my_col = lax.axis_index("row"), lax.axis_index("col")
    n_row, n_col = lax.axis_size("row"), lax.axis_size("col")

    def exists(dr, dc):
        row, col = my_row + dr, my_col + dc
        ok = None
        for spot, count, delta in ((row, n_row, dr), (col, n_col, dc)):
            if delta:
                here = (spot >= 0) & (spot < count)
                ok = here if ok is None else ok & here
        return ok

    own = pl.ds(TOP, ROWS)
    pairs = [(k_hbm, k_ref), (wave_hbm, wave_ref)]
    pairs += [(cap_hbm, cap_ref), (shunt_hbm, shunt_ref), (tap_hbm, tap_ref), (mask_hbm, mask_ref)]
    for p in range(2):
        cols = pl.ds(p * LANES, LANES)
        pairs.append((v_hbm.at[:, cols], v_ref.at[p + 1, own, :]))
        for comp in range(2):
            pairs.append((c_hbm.at[comp, :, cols], c_ref.at[comp, p + 1, own, :]))
            pairs.append((r_hbm.at[comp, :, cols], r_ref.at[comp, p + 1, own, :]))
    loads = [pltpu.make_async_copy(src, dst, load_sem.at[i]) for i, (src, dst) in enumerate(pairs)]
    barrier = pltpu.get_barrier_semaphore()
    for dr, dc in DIRECTIONS:
        @pl.when(exists(dr, dc))
        def _(dr=dr, dc=dc):
            pl.semaphore_signal(barrier, inc=1, device_id=(my_row + dr, my_col + dc), device_id_type=MESH)

    for one in loads:
        one.start()
    has_up, has_down, has_left, has_right = (exists(*d) for d in DIRECTIONS[:4])

    for side, missing in enumerate((has_up, has_down)):
        @pl.when(jnp.logical_not(missing))
        def _(side=side):
            fromv_ref[side] = jnp.zeros(fromv_ref.shape[1:], BF16)
            rows = pl.ds(0, TOP) if side == 0 else pl.ds(TOP + ROWS, TOP)
            for other in range(2):
                froms_ref[other, rows, :] = jnp.zeros((TOP, COLS), BF16)

    for side, missing in enumerate((has_left, has_right)):
        @pl.when(jnp.logical_not(missing))
        def _(side=side):
            froms_ref[side] = jnp.zeros(froms_ref.shape[1:], BF16)

    def message(which):
        dr, dc = DIRECTIONS[which]
        low, mid, high = pl.ds(0, TOP), pl.ds(TOP, ROWS), pl.ds(TOP + ROWS, TOP)
        first, last = pl.ds(0, TOP), pl.ds(ROWS - TOP, TOP)
        if dc == 0:
            side = 0 if dr > 0 else 1
            source, target = sendv_ref.at[1 - side], fromv_ref.at[side]
        else:
            side = 0 if dc > 0 else 1
            out, land = sends_ref.at[1 - side], froms_ref.at[side]
            source = out if dr == 0 else out.at[first if dr < 0 else last, :]
            target = land.at[mid if dr == 0 else (high if dr < 0 else low), :]
        return pltpu.make_async_remote_copy(
            src_ref=source,
            dst_ref=target,
            send_sem=send_sem.at[which],
            recv_sem=recv_sem.at[which],
            device_id=(my_row + dr, my_col + dc),
            device_id_type=MESH,
        )

    def prepare():
        n = 32
        for lo in range(0, ROWS, n):
            rows, at = pl.ds(lo, n), pl.ds(TOP + lo, n)
            for p in range(2):
                cols = slice(p * LANES, (p + 1) * LANES)
                tap = tap_ref[rows, cols]
                for step in range(STEPS):
                    value = jnp.zeros(tap.shape, F32)
                    for which in range(NW):
                        value = jnp.where(tap == which, wave_ref[step, which], value)
                    load_ref[step, rows, cols] = value
                v = v_ref[p + 1, at, :]
                cap = cap_ref[rows, cols]
                held = mask_ref[rows, cols] == 1
                b = jnp.where(held, 0.0, cap)
                q = jnp.where(held, 0.0, cap * (load_ref[0, rows, cols] - shunt_ref[rows, cols] * v))
                b_ref[p + 1, at, :] = b
                q_ref[p + 1, at, :] = q
                part = {"b": b, "q": q}
                for comp in range(2):
                    c, r = c_ref[comp, p + 1, at, :], r_ref[comp, p + 1, at, :]
                    w = r * c
                    w_ref[comp, p + 1, at, :] = w
                    part["c%d" % comp], part["r%d" % comp], part["w%d" % comp] = c, r, w
                part["vh"] = v.astype(BF16).astype(F32)
                part["vl"] = v - part["vh"]
                lane = lane_of((n, LANES))
                for tile, names in enumerate(LANE_TILES):
                    mixed = None
                    for name, base in reversed(list(lane_slots(names))):
                        turned = roll(part[name], base if p == 0 else base + WIDTH[name])
                        mixed = turned if mixed is None else jnp.where(lane < base + WIDTH[name], turned, mixed)
                    sends_ref[p, rows, tile * LANES : (tile + 1) * LANES] = mixed.astype(BF16)

    def stack():
        for p in range(2):
            cols = slice(p * LANES, (p + 1) * LANES)
            for side in range(2):
                for name, width in SLOTS:
                    at = pl.ds(TOP if side == 0 else TOP + ROWS - width, width)
                    if name[0] == "v":
                        v = v_ref[p + 1, at, :]
                        value = v.astype(BF16).astype(F32)
                        value = value if name == "vh" else v - value
                    elif name in ("b", "q"):
                        value = (b_ref if name == "b" else q_ref)[p + 1, at, :]
                    else:
                        ref = {"w": w_ref, "c": c_ref, "r": r_ref}[name[0]]
                        value = ref[int(name[1]), p + 1, at, :]
                    stage_ref[side, pl.ds(ROW_BASE[name], width), cols] = value
        for side in range(2):
            for lo in range(0, 256, 64):
                sendv_ref[side, pl.ds(lo, 64), :] = stage_ref[side, pl.ds(lo, 64), :].astype(BF16)

    def put(name, tile, at, value):
        if name in ("b", "q"):
            (b_ref if name == "b" else q_ref)[tile, at, :] = value
        else:
            ref = {"w": w_ref, "c": c_ref, "r": r_ref}[name[0]]
            ref[int(name[1]), tile, at, :] = value

    def unpack_sides(first, last, n):
        for side in range(2):
            tile = 3 * side
            for lo in range(first, last, n):
                at = pl.ds(lo, n)
                near = lo + n > FROM and lo < EXT - FROM
                got = {}
                for half, names in enumerate(LANE_TILES):
                    value = froms_ref[side, at, half * LANES : (half + 1) * LANES].astype(F32)
                    for name, base in lane_slots(names):
                        if WIDTH[name] == NEAR and not near:
                            continue
                        got[name] = roll(value, -(base + WIDTH[name]) if side == 0 else -base)
                v_ref[tile, at, :] = got["vh"] + got["vl"]
                for name in got:
                    if name[0] != "v":
                        put(name, tile, at, got[name])

    def unpack_ends():
        for side in range(2):
            for lo in range(0, 256, 64):
                stage_ref[side, pl.ds(lo, 64), :] = fromv_ref[side, pl.ds(lo, 64), :].astype(F32)
            for p in range(2):
                cols = slice(p * LANES, (p + 1) * LANES)
                for name, width in SLOTS:
                    at = pl.ds(TOP - width if side == 0 else TOP + ROWS, width)
                    value = stage_ref[side, pl.ds(ROW_BASE[name], width), cols]
                    if name == "vh":
                        v_ref[p + 1, at, :] = value + stage_ref[side, pl.ds(ROW_BASE["vl"], width), cols]
                    elif name != "vl":
                        put(name, p + 1, at, value)

    def windows(tiles, nexts, wanted):
        lane = lane_of(tiles[0].shape)
        mark, low = lane & 63, lane < 64
        pair = {}
        for at in range(4):
            crossed = roll(jnp.where(low, nexts[at], tiles[at]), 64)
            if at > 0:
                pair[2 * at - 2] = jnp.where(low, tiles[at], crossed)
            if at < 3:
                pair[2 * at - 1] = jnp.where(low, crossed, nexts[at])
        out = {}
        for k in wanted:
            i = k // 2
            if k % 2 == 0:
                out[k] = jnp.where(mark < 48, pair[i], pair[i - 1])
            else:
                out[k] = jnp.where(mark < 16, pair[i + 1], pair[i])
        return out

    def driving(step, comp, base, n):
        reach = WIDE if step == 0 else NEAR - 1
        lo = jnp.where(has_up, TOP - reach, TOP)
        hi = jnp.where(has_down, TOP + ROWS + reach - 1, TOP + ROWS)
        at, nxt = pl.ds(base, n), pl.ds(base + 1, n)
        row = lax.broadcasted_iota(jnp.int32, (n, LANES), 0) + base
        lane = lane_of((n, LANES))
        inside = (row >= lo) & (row < hi)
        held = [inside & has_left, inside, inside, inside & has_right]
        v = [v_ref[k, at, :] for k in range(4)]
        out = []
        for k in range(4):
            if step == 0:
                w = w_ref[comp, k, at, :]
            else:
                w = r_ref[comp, k, at, :] * c_ref[comp, k, at, :]
            if comp == 0:
                beside = v_ref[k, nxt, :]
            else:
                beside = roll(jnp.where(lane == 0, v[min(k + 1, 3)], v[k]), LANES - 1)
            out.append(jnp.where(held[k], v[k] - beside - w, 0.0))
        return out

    def drive(step, comp, start, stop):
        n = 16
        carried = None
        if stop < EXT - SKIP:
            carried = driving(step, comp, stop, 8)
        for base in reversed(range(start, stop, n)):
            size = min(n, stop - base)
            out = driving(step, comp, base, size)
            nexts = []
            for k in range(4):
                after = out[k][0:8] if carried is None else carried[k]
                nexts.append(pltpu.roll(jnp.concatenate([out[k], after], axis=0), size + 7, 0)[0:size])
            carried = [one[0:8] for one in out]
            for k, value in windows(out, nexts, blocks_of(step, comp)).items():
                for g in range(size // 8):
                    spot = pl.ds((base - SKIP) // 8 + g, 8, stride=PITCH)
                    drive_ref[10 * comp + k + 1, spot, :] = value[8 * g : 8 * g + 8]

    def blocks_of(step, comp):
        if step == 0:
            return tuple(range(-1, 9))
        return tuple(range(0, 8)) if comp == 0 else tuple(range(-1, 8))

    def convolve(step, comp):
        blocks = blocks_of(step, comp)
        start, n = (0, 24) if step == 0 else ((16, 24) if comp == 0 else (24, 16))
        part = [{}, {}]
        for odd in range(2):
            mine = [k for k in blocks if k % 2 == odd]
            columns = []
            for chunk in range(CHUNKS):
                group, phase = divmod(2 * chunk, 8)
                at = pl.ds(phase * PITCH + start // 8 + group, n)
                columns.append(jnp.concatenate([drive_ref[10 * comp + 1 + k, at, :] for k in mine], axis=0).astype(BF16))
            if odd:
                order = [(i ^ 1) * 32 for i in range(DEPTH // 32)]
                weights = jnp.concatenate([table_ref[comp, lo : lo + 32, :] for lo in order], axis=0)
            else:
                weights = table_ref[comp]
            product = jnp.dot(jnp.concatenate(columns, axis=1), weights, preferred_element_type=F32)
            for i, k in enumerate(mine):
                for side in range(2):
                    part[side][k] = product[i * n : (i + 1) * n, side * LANES : (side + 1) * LANES]
        lane = lane_of((n, LANES))

        def chosen(options):
            value = None
            for group in reversed(range(4)):
                if options[group] is not None:
                    value = options[group] if value is None else jnp.where(lane < STRIP * (group + 1), options[group], value)
            return value

        for side in range(2):
            for tile in range(4):
                held = [part[side].get(4 * (tile - 1) + q) for q in range(4)]
                if all(one is None for one in held):
                    continue
                moved = []
                for d in range(4):
                    value = chosen([held[(t + d) % 4] for t in range(4)])
                    moved.append(roll(value, STRIP * d) if d else value)
                for t in range(4):
                    value = chosen([None if held[q] is None else moved[(q - t) % 4] for q in range(4)])
                    flow_ref[comp, tile, pl.ds((4 * side + t) * FLOW + start // 8, n), :] = value

    def flow(comp, tile, first, n):
        parts = [flow_ref[comp, tile, pl.ds(first // 8 + g, 8, stride=FLOW), :] for g in range(n // 8)]
        return jnp.concatenate(parts, axis=0) if len(parts) > 1 else parts[0]

    def advance_frame():
        n = 16
        lo = jnp.where(has_up, 0, TOP)
        hi = jnp.where(has_down, EXT, TOP + ROWS)
        for base in range(FROM, EXT - FROM, n):
            at = pl.ds(base, n)
            row = lax.broadcasted_iota(jnp.int32, (n, LANES), 0) + base
            inside = (row >= lo) & (row < hi)
            held = [inside & has_left, inside, inside, inside & has_right]
            for comp in range(2):
                for k in range(4):
                    value = c_ref[comp, k, at, :] + flow(comp, k, base - FROM, n)
                    c_ref[comp, k, at, :] = jnp.where(held[k], value, 0.0)

    def divergence(base, n, k):
        at = pl.ds(base, n)
        lane = lane_of((n, LANES))
        c1 = c_ref[1, k, at, :]
        before_x = c_ref[0, k, pl.ds(base - 1, n), :]
        before_y = roll(jnp.where(lane == LANES - 1, c_ref[1, max(k - 1, 0), at, :], c1), 1)
        return c_ref[0, k, at, :] - before_x + c1 - before_y

    def update_frame():
        n = 16
        for base in range(FROM, EXT - FROM, n):
            at = pl.ds(base, n)
            for k in range(4):
                b = b_ref[k, at, :]
                value = v_ref[k, at, :] + q_ref[k, at, :] - b * divergence(base, n, k)
                v_ref[k, at, :] = jnp.where(b == 0.0, 0.0, value)

    def finish():
        n = 32
        for k in range(1, 3):
            at = pl.ds(TOP - 8, 8)
            head = c_ref[0, k, at, :] + flow(0, k, TOP - 8 - FROM, 8)
            c_ref[0, k, at, :] = jnp.where(has_up, head, 0.0)
        for lo in range(0, ROWS, n):
            at, first = pl.ds(TOP + lo, n), TOP + lo - FROM
            left = c_ref[1, 0, at, :] + flow(1, 0, first, n)
            c_ref[1, 0, at, :] = jnp.where(has_left, left, 0.0)
            for k in range(1, 3):
                cols = slice((k - 1) * LANES, k * LANES)
                for comp in range(2):
                    value = c_ref[comp, k, at, :] + flow(comp, k, first, n)
                    c_ref[comp, k, at, :] = value
                    cout_ref[comp, pl.ds(lo, n), cols] = value
        for lo in range(0, ROWS, n):
            at, rows = pl.ds(TOP + lo, n), pl.ds(lo, n)
            for k in range(1, 3):
                cols = slice((k - 1) * LANES, k * LANES)
                v = v_ref[k, at, :]
                change = load_ref[1, rows, cols] - divergence(TOP + lo, n, k) - shunt_ref[rows, cols] * v
                vout_ref[rows, cols] = jnp.where(mask_ref[rows, cols] == 1, 0.0, v + cap_ref[rows, cols] * change)

    for one in loads:
        one.wait()
    prepare()
    stack()
    pl.semaphore_wait(barrier, (1 + one_if(has_up) + one_if(has_down)) * (1 + one_if(has_left) + one_if(has_right)) - 1)
    for which, (dr, dc) in enumerate(DIRECTIONS):
        @pl.when(exists(dr, dc))
        def _(which=which):
            message(which).start()
    build_table(k_ref, pad_ref, base_ref, table_ref)
    def receive(wanted):
        for which in wanted:
            dr, dc = DIRECTIONS[which]

            @pl.when(exists(-dr, -dc))
            def _(which=which):
                message(which).wait_recv()

    low, high = TOP, TOP + ROWS
    receive((0, 1))
    unpack_ends()
    receive((2, 3))
    unpack_sides(low, high, 16)
    for comp in range(2):
        drive(0, comp, low, high - 16)
    receive((4, 5, 6, 7))
    unpack_sides(SKIP, low, 8)
    unpack_sides(high, EXT - SKIP, 8)
    for comp in range(2):
        drive(0, comp, high - 16, EXT - SKIP)
        drive(0, comp, SKIP, low)
        convolve(0, comp)
    advance_frame()
    update_frame()
    for comp in range(2):
        drive(1, comp, FROM, EXT - FROM)
        convolve(1, comp)
    finish()
    for which, (dr, dc) in enumerate(DIRECTIONS):
        @pl.when(exists(dr, dc))
        def _(which=which):
            message(which).wait_send()


def local(voltage, currents, resistance, inverse_cap, shunt_conductance, tap_index, pad_mask, waveforms, k_window):
    hbm = pl.BlockSpec(memory_space=pltpu.HBM)
    vmem = pl.BlockSpec(memory_space=pltpu.VMEM)
    block = (ROWS, COLS)
    frame = (4, EXT, LANES)
    scratch = [
        pltpu.VMEM(block, F32),
        pltpu.VMEM(block, F32),
        pltpu.VMEM(block, jnp.int32),
        pltpu.VMEM(block, jnp.int32),
        pltpu.VMEM(frame, F32),
        pltpu.VMEM((2, *frame), F32),
        pltpu.VMEM((2, *frame), F32),
        pltpu.VMEM((2, *frame), F32),
        pltpu.VMEM(frame, F32),
        pltpu.VMEM(frame, F32),
        pltpu.VMEM((2, 256, COLS), F32),
        pltpu.VMEM((2, 256, COLS), BF16),
        pltpu.VMEM((2, ROWS, COLS), BF16),
        pltpu.VMEM((2, 256, COLS), BF16),
        pltpu.VMEM((2, EXT, COLS), BF16),
        pltpu.VMEM((20, 8 * PITCH, LANES), F32),
        pltpu.VMEM((2, DEPTH, 2 * LANES), BF16),
        pltpu.VMEM((2, 48, LANES), F32),
        pltpu.VMEM((2, 2, 40, LANES), F32),
        pltpu.VMEM((STEPS, *block), F32),
        pltpu.VMEM((2, 4, 8 * FLOW, LANES), F32),
        pltpu.SMEM((STEPS, NW), F32),
        pltpu.VMEM((SPAN, 2, SPAN), BF16),
        pltpu.SemaphoreType.DMA((16,)),
        pltpu.SemaphoreType.DMA((8,)),
        pltpu.SemaphoreType.DMA((8,)),
    ]
    call = pl.pallas_call(
        kernel,
        out_shape=(jax.ShapeDtypeStruct(block, F32), jax.ShapeDtypeStruct((2, *block), F32)),
        in_specs=[hbm] * 9,
        out_specs=(vmem, vmem),
        scratch_shapes=scratch,
        compiler_params=pltpu.CompilerParams(
            collective_id=0, has_side_effects=True, vmem_limit_bytes=40 * 1024 * 1024
        ),
    )
    held = [waveforms, jnp.transpose(k_window, (1, 0, 2)), voltage, currents, resistance, inverse_cap]
    held += [shunt_conductance, tap_index, pad_mask]
    held = [pltpu.with_memory_space_constraint(one, pltpu.HBM) for one in held]
    voltage_new, currents_new = call(*held)

    def copy_out(v_ref, c_ref, vout_hbm, cout_hbm, sem):
        copies = [pltpu.make_async_copy(v_ref, vout_hbm, sem.at[0]), pltpu.make_async_copy(c_ref, cout_hbm, sem.at[1])]
        for one in copies:
            one.start()
        for one in copies:
            one.wait()

    return pl.pallas_call(
        copy_out,
        out_shape=(jax.ShapeDtypeStruct(block, F32), jax.ShapeDtypeStruct((2, *block), F32)),
        in_specs=[vmem, vmem],
        out_specs=(hbm, hbm),
        scratch_shapes=[pltpu.SemaphoreType.DMA((2,))],
        compiler_params=pltpu.CompilerParams(vmem_limit_bytes=1024 * 1024),
    )(voltage_new, currents_new)


def solution(mesh):
    placed = (
        P("row", "col"),
        P(None, "row", "col"),
        P(None, "row", "col"),
        P("row", "col"),
        P("row", "col"),
        P("row", "col"),
        P("row", "col"),
        P(),
        P(),
    )
    return jax.shard_map(
        local,
        mesh=mesh,
        in_specs=placed,
        out_specs=(P("row", "col"), P(None, "row", "col")),
        check_vma=False,
    )
```
